64 devices in a mesh: dp: 8 (over x, y, core), tp: 8 (over z).
Axes of the slice: x: 2, y: 2, z: 8, core: 2. Of those that a mesh axis runs over, the one named last changes fastest.
The devices are a block of a 4x4x8 slice.
Arguments:
- x: bfloat16 [16384, 4096], P('dp'), parts along dimension 0
- w_gate: bfloat16 [4096, 16384], P(None, 'tp')
- w_up: bfloat16 [4096, 16384], P(None, 'tp')
- w_down: bfloat16 [16384, 4096], P('tp')
Outputs:
- output: bfloat16 [16384, 4096], P('dp'), parts along dimension 0
There are 8 independent parts. The reference program is written for one: setup_inputs(seed, part) draws one part's arguments, and reference() takes and returns one part's arrays. A program takes and returns all parts, laid end to end along the dimension named above; an argument that names none is the same for every part.
All inputs are finite; a program needn't handle non-finite values.
Results may differ from the reference program's by a relative error of at most 0.016.
Values are sent between devices in bfloat16 or wider.
A program may use at most 768 MiB of HBM per device.

```python
import jax
import jax.numpy as jnp

ROWS = 2048
D = 4096
FF = 16384


def setup_inputs(seed: int = 0, part: int = 0) -> dict:
    kx, kg, ku, kd = jax.random.split(jax.random.key(seed), 4)
    drawn = {
        "x": jax.random.normal(jax.random.fold_in(kx, part), (ROWS, D), jnp.float32),
        "w_gate": jax.random.normal(kg, (D, FF), jnp.float32) * D**-0.5,
        "w_up": jax.random.normal(ku, (D, FF), jnp.float32) * D**-0.5,
        "w_down": jax.random.normal(kd, (FF, D), jnp.float32) * FF**-0.5,
    }
    return {k: v.astype(jnp.bfloat16) for k, v in drawn.items()}


def reference(x, w_gate, w_up, w_down):
    gate = jnp.dot(x, w_gate, preferred_element_type=jnp.float32)
    up = jnp.dot(x, w_up, preferred_element_type=jnp.float32)
    hidden = (jax.nn.silu(gate) * up).astype(jnp.bfloat16)
    return jnp.dot(hidden, w_down, preferred_element_type=jnp.float32).astype(jnp.bfloat16)
```

```python
import functools

import jax
import jax.numpy as jnp
from jax import lax
from jax.experimental import pallas as pl
from jax.experimental.pallas import tpu as pltpu
from jax.sharding import PartitionSpec as P

MESH = pl.DeviceIdType.MESH
FB = 256
DB = 512


def ring_kernel(
    n, x, wg, wu, wd, y, wgv, wuv, wdv, xv, hv, tv, land, out,
    w_sem, d_sem, x_sem, send_rs, recv_rs, send_ag, recv_ag, y_sem,
):
    me = lax.axis_index("tp")
    rows, cols = x.shape
    hidden = wg.shape[1]
    half = rows // 2
    rb = half // n
    nj, nc = hidden // FB, cols // DB
    peers = (lax.rem(me + 1, n), lax.rem(me + n - 1, n))

    def block_rows(d, s):
        b = lax.rem(me + 2 * n - s, n) if d == 0 else lax.rem(me + s, n)
        return pl.ds(pl.multiple_of(d * half + b * rb, rb), rb)

    def columns(i, size):
        return pl.ds(pl.multiple_of(i * size, size), size)

    def load_w(j):
        c = columns(j, FB)
        return (
            pltpu.make_async_copy(wg.at[:, c], wgv.at[:, c], w_sem.at[0, j]),
            pltpu.make_async_copy(wu.at[:, c], wuv.at[:, c], w_sem.at[1, j]),
        )

    def load_d(c):
        k = columns(c, DB)
        return pltpu.make_async_copy(wd.at[:, k], wdv.at[:, k], d_sem.at[c])

    def load_x(d, s):
        return pltpu.make_async_copy(
            x.at[block_rows(d, s), :], xv.at[pl.ds(d * rb, rb), :], x_sem.at[d]
        )

    def remote(src, dst, ssem, rsem, d):
        return pltpu.make_async_remote_copy(
            src_ref=src, dst_ref=dst, send_sem=ssem, recv_sem=rsem,
            device_id={"tp": peers[d]}, device_id_type=MESH,
        )

    def hop(d, s, c):
        now, later = lax.rem(s, 2), lax.rem(s + 1, 2)
        return remote(
            out.at[d, now, c], land.at[d, later, c],
            send_rs.at[d, now, c], recv_rs.at[d, later, c], d,
        )

    def gather_hop(d, t, c):
        there = y.at[block_rows(d, n - 1 + t), columns(c, DB)]
        return remote(there, there, send_ag.at[d, t, c], recv_ag.at[d, t, c], d)

    def first_gather_hop(d, c):
        there = y.at[block_rows(d, n - 1), columns(c, DB)]
        return remote(
            out.at[d, (n - 1) % 2, c], there, send_ag.at[d, 0, c], recv_ag.at[d, 0, c], d
        )

    def keep(d, c):
        return pltpu.make_async_copy(
            out.at[d, (n - 1) % 2, c],
            y.at[block_rows(d, n - 1), columns(c, DB)],
            y_sem.at[d, c],
        )

    for d in range(2):
        load_x(d, 0).start()
    for j in range(2):
        for copy in load_w(j):
            copy.start()

    barrier = pltpu.get_barrier_semaphore()
    for peer in peers:
        pl.semaphore_signal(barrier, inc=1, device_id={"tp": peer}, device_id_type=MESH)
    pl.semaphore_wait(barrier, 2)

    def ring_step(s, _):
        for d in range(2):
            load_x(d, s).wait()

        def gate_up(j, _):
            @pl.when(s == 0)
            def _():
                for copy in load_w(j):
                    copy.wait()

                @pl.when(j + 2 < nj)
                def _():
                    for copy in load_w(j + 2):
                        copy.start()

                @pl.when(j + 2 >= nj)
                def _():
                    for i in range(nc // 2):
                        load_d((j + 2 - nj) * (nc // 2) + i).start()

            k = columns(j, FB)
            gate = jnp.dot(xv[...], wgv[:, k], preferred_element_type=jnp.float32)
            up = jnp.dot(xv[...], wuv[:, k], preferred_element_type=jnp.float32)
            hv[:, k] = (jax.nn.silu(gate) * up).astype(jnp.bfloat16)
            return 0

        lax.fori_loop(0, nj, gate_up, 0)

        @pl.when(s < n - 1)
        def _():
            for d in range(2):
                load_x(d, s + 1).start()

        now = lax.rem(s, 2)

        def down(c, _):
            @pl.when(s == 0)
            def _():
                load_d(c).wait()

            tv[...] = jnp.dot(hv[...], wdv[:, columns(c, DB)], preferred_element_type=jnp.float32)

            @pl.when(s >= 2)
            def _():
                for d in range(2):
                    hop(d, s - 2, c).wait_send()

            @pl.when(s == 0)
            def _():
                for d in range(2):
                    out[d, now, c] = tv[d * rb:(d + 1) * rb, :].astype(jnp.bfloat16)

            @pl.when(s > 0)
            def _():
                for d in range(2):
                    hop(d, s - 1, c).wait_recv()
                for d in range(2):
                    total = land[d, now, c].astype(jnp.float32) + tv[d * rb:(d + 1) * rb, :]
                    out[d, now, c] = total.astype(jnp.bfloat16)

            @pl.when(s < n - 1)
            def _():
                for d in range(2):
                    hop(d, s, c).start()

            @pl.when(s == n - 1)
            def _():
                for d in range(2):
                    first_gather_hop(d, c).start()
                for d in range(2):
                    keep(d, c).start()

            return 0

        lax.fori_loop(0, nc, down, 0)
        return 0

    lax.fori_loop(0, n, ring_step, 0)

    def gather_step(t, _):
        def piece(c, _):
            for d in range(2):
                gather_hop(d, t, c).wait_recv()

                @pl.when(t < n - 2)
                def _():
                    gather_hop(d, t + 1, c).start()

            return 0

        return lax.fori_loop(0, nc, piece, 0)

    lax.fori_loop(0, n - 1, gather_step, 0)

    def finish(c, _):
        for d in range(2):
            hop(d, n - 2, c).wait_send()
            first_gather_hop(d, c).wait_send()
            keep(d, c).wait()

            def sent(t, _):
                gather_hop(d, t, c).wait_send()
                return 0

            lax.fori_loop(1, n - 1, sent, 0)
        return 0

    lax.fori_loop(0, nc, finish, 0)


def solution(mesh):
    n = mesh.shape["tp"]

    def step(x, w_gate, w_up, w_down):
        rows, cols = x.shape
        hidden = w_gate.shape[1]
        rb = rows // 2 // n
        nj, nc = hidden // FB, cols // DB
        dma = pltpu.SemaphoreType.DMA
        return pl.pallas_call(
            functools.partial(ring_kernel, n),
            name="mlp_ring",
            out_shape=jax.ShapeDtypeStruct((rows, cols), jnp.bfloat16),
            in_specs=[pl.BlockSpec(memory_space=pl.ANY)] * 4,
            out_specs=pl.BlockSpec(memory_space=pl.ANY),
            scratch_shapes=[
                pltpu.VMEM(w_gate.shape, jnp.bfloat16),
                pltpu.VMEM(w_up.shape, jnp.bfloat16),
                pltpu.VMEM(w_down.shape, jnp.bfloat16),
                pltpu.VMEM((2 * rb, cols), jnp.bfloat16),
                pltpu.VMEM((2 * rb, hidden), jnp.bfloat16),
                pltpu.VMEM((2 * rb, DB), jnp.float32),
                pltpu.VMEM((2, 2, nc, rb, DB), jnp.bfloat16),
                pltpu.VMEM((2, 2, nc, rb, DB), jnp.bfloat16),
                dma((2, nj)),
                dma((nc,)),
                dma((2,)),
                dma((2, 2, nc)),
                dma((2, 2, nc)),
                dma((2, n - 1, nc)),
                dma((2, n - 1, nc)),
                dma((2, nc)),
            ],
            compiler_params=pltpu.CompilerParams(
                collective_id=0, has_side_effects=True, vmem_limit_bytes=67043328
            ),
        )(x, w_gate, w_up, w_down)

    return jax.shard_map(
        step,
        mesh=mesh,
        in_specs=(P("dp", None), P(None, "tp"), P(None, "tp"), P("tp", None)),
        out_specs=P("dp", None),
        check_vma=False,
    )
```

```python
import functools

import jax
import jax.numpy as jnp
from jax import lax
from jax.experimental import pallas as pl
from jax.experimental.pallas import tpu as pltpu
from jax.sharding import PartitionSpec as P

MESH = pl.DeviceIdType.MESH
FB = 256
DB = 1024
AHEAD = 2


def ring_kernel(
    n, x, wg, wu, wd, held, wuv, wdv, xv, hv, tv, land, out,
    w_sem, d_sem, x_sem, send_rs, recv_rs, send_ag, recv_ag, free_sem,
):
    me = lax.axis_index("tp")
    rows, cols = x.shape
    hidden = wg.shape[1]
    half = rows // 2
    rb = half // n
    nj, nc, strips = hidden // FB, cols // DB, DB // FB
    peers = (lax.rem(me + 1, n), lax.rem(me + n - 1, n))

    def block(d, s):
        return lax.rem(me + 2 * n - s, n) if d == 0 else lax.rem(me + s, n)

    def span(i, size):
        return pl.ds(pl.multiple_of(i * size, size), size)

    def load_w(j):
        k = span(j, FB)
        return (
            pltpu.make_async_copy(wg.at[:, k], held.at[span(j, cols), :], w_sem.at[0, j]),
            pltpu.make_async_copy(wu.at[:, k], wuv.at[:, k], w_sem.at[1, j]),
        )

    def load_d(c):
        k = span(c, DB)
        return pltpu.make_async_copy(wd.at[:, k], wdv.at[:, k], d_sem.at[c])

    def load_x(d, s):
        start = pl.multiple_of(d * half + block(d, s) * rb, rb)
        return pltpu.make_async_copy(
            x.at[pl.ds(start, rb), :], xv.at[pl.ds(d * rb, rb), :], x_sem.at[d]
        )

    def remote(src, dst, ssem, rsem, d):
        return pltpu.make_async_remote_copy(
            src_ref=src, dst_ref=dst, send_sem=ssem, recv_sem=rsem,
            device_id={"tp": peers[d]}, device_id_type=MESH,
        )

    def hop(d, s, c):
        now, later = lax.rem(s, 2), lax.rem(s + 1, 2)
        return remote(
            out.at[d, now, c], land.at[d, later, c],
            send_rs.at[d, now, c], recv_rs.at[d, later, c], d,
        )

    def piece_start(d, s, c):
        return ((d * n + block(d, s)) * nc + c) * (strips * rb)

    def gather_hop(d, t, c):
        p = held.at[pl.ds(pl.multiple_of(piece_start(d, n - 1 + t, c), rb), strips * rb), :]
        return remote(p, p, send_ag.at[d, t, c], recv_ag.at[d, t, c], d)

    for d in range(2):
        load_x(d, 0).start()
    for j in range(AHEAD):
        for copy in load_w(j):
            copy.start()

    barrier = pltpu.get_barrier_semaphore()
    for peer in peers:
        pl.semaphore_signal(barrier, inc=1, device_id={"tp": peer}, device_id_type=MESH)
    pl.semaphore_wait(barrier, 2)

    def ring_step(s, _):
        for d in range(2):
            load_x(d, s).wait()

        def gate_up(j, _):
            @pl.when(s == 0)
            def _():
                for copy in load_w(j):
                    copy.wait()

                @pl.when(j + AHEAD < nj)
                def _():
                    for copy in load_w(j + AHEAD):
                        copy.start()

                @pl.when(j + AHEAD >= nj)
                def _():
                    for i in range(nc // AHEAD):
                        load_d((j + AHEAD - nj) * (nc // AHEAD) + i).start()

            gate = jnp.dot(xv[...], held[span(j, cols), :], preferred_element_type=jnp.float32)
            up = jnp.dot(xv[...], wuv[:, span(j, FB)], preferred_element_type=jnp.float32)
            hv[:, span(j, FB)] = (jax.nn.silu(gate) * up).astype(jnp.bfloat16)
            return 0

        lax.fori_loop(0, nj, gate_up, 0)

        @pl.when(s < n - 1)
        def _():
            for d in range(2):
                load_x(d, s + 1).start()

        @pl.when(s == n - 1)
        def _():
            for peer in peers:
                pl.semaphore_signal(free_sem, inc=1, device_id={"tp": peer}, device_id_type=MESH)
            pl.semaphore_wait(free_sem, 2)

        now = lax.rem(s, 2)

        def down(c, _):
            @pl.when(s == 0)
            def _():
                load_d(c).wait()

            tv[...] = jnp.dot(hv[...], wdv[:, span(c, DB)], preferred_element_type=jnp.float32)

            def term(d, i):
                return tv[d * rb:(d + 1) * rb, i * FB:(i + 1) * FB]

            def arrived(d, i):
                return land[d, now, c, i * rb:(i + 1) * rb, :].astype(jnp.float32)

            @pl.when((s >= 2) & (s < n - 1))
            def _():
                for d in range(2):
                    hop(d, s - 2, c).wait_send()

            @pl.when(s > 0)
            def _():
                for d in range(2):
                    hop(d, s - 1, c).wait_recv()

            @pl.when(s == 0)
            def _():
                for d in range(2):
                    for i in range(strips):
                        out[d, now, c, i * rb:(i + 1) * rb, :] = term(d, i).astype(jnp.bfloat16)

            @pl.when((s > 0) & (s < n - 1))
            def _():
                for d in range(2):
                    for i in range(strips):
                        total = arrived(d, i) + term(d, i)
                        out[d, now, c, i * rb:(i + 1) * rb, :] = total.astype(jnp.bfloat16)

            @pl.when(s < n - 1)
            def _():
                for d in range(2):
                    hop(d, s, c).start()

            @pl.when(s == n - 1)
            def _():
                for d in range(2):
                    for i in range(strips):
                        start = pl.multiple_of(piece_start(d, n - 1, c) + i * rb, rb)
                        total = arrived(d, i) + term(d, i)
                        held[pl.ds(start, rb), :] = total.astype(jnp.bfloat16)
                for d in range(2):
                    gather_hop(d, 0, c).start()

            return 0

        lax.fori_loop(0, nc, down, 0)
        return 0

    lax.fori_loop(0, n, ring_step, 0)

    def gather_step(t, _):
        def piece(c, _):
            for d in range(2):
                gather_hop(d, t, c).wait_recv()

                @pl.when(t < n - 2)
                def _():
                    gather_hop(d, t + 1, c).start()

            return 0

        return lax.fori_loop(0, nc, piece, 0)

    lax.fori_loop(0, n - 1, gather_step, 0)

    def finish(c, _):
        for d in range(2):
            hop(d, n - 3, c).wait_send()
            hop(d, n - 2, c).wait_send()

            def sent(t, _):
                gather_hop(d, t, c).wait_send()
                return 0

            lax.fori_loop(0, n - 1, sent, 0)
        return 0

    lax.fori_loop(0, nc, finish, 0)


def place_kernel(n, held, y, sem):
    rows, cols = y.shape
    rb = rows // 2 // n
    nk = cols // FB

    def copy(i):
        r, k = lax.div(i, nk), lax.rem(i, nk)
        return pltpu.make_async_copy(
            held.at[pl.ds(pl.multiple_of(i * rb, rb), rb), :],
            y.at[pl.ds(pl.multiple_of(r * rb, rb), rb), pl.ds(pl.multiple_of(k * FB, FB), FB)],
            sem.at[i],
        )

    def start(i, _):
        copy(i).start()
        return 0

    def wait(i, _):
        copy(i).wait()
        return 0

    lax.fori_loop(0, 2 * n * nk, start, 0)
    lax.fori_loop(0, 2 * n * nk, wait, 0)


def solution(mesh):
    n = mesh.shape["tp"]

    def step(x, w_gate, w_up, w_down):
        rows, cols = x.shape
        hidden = w_gate.shape[1]
        rb = rows // 2 // n
        nj, nc = hidden // FB, cols // DB
        dma = pltpu.SemaphoreType.DMA
        bf16 = jnp.bfloat16
        held = pl.pallas_call(
            functools.partial(ring_kernel, n),
            name="mlp_ring",
            out_shape=pltpu.VMEM((max(rows, hidden) * cols // FB, FB), bf16),
            in_specs=[pl.BlockSpec(memory_space=pl.ANY)] * 4,
            out_specs=pl.BlockSpec(memory_space=pltpu.VMEM),
            scratch_shapes=[
                pltpu.VMEM(w_up.shape, bf16),
                pltpu.VMEM(w_down.shape, bf16),
                pltpu.VMEM((2 * rb, cols), bf16),
                pltpu.VMEM((2 * rb, hidden), bf16),
                pltpu.VMEM((2 * rb, DB), jnp.float32),
                pltpu.VMEM((2, 2, nc, rb * DB // FB, FB), bf16),
                pltpu.VMEM((2, 2, nc, rb * DB // FB, FB), bf16),
                dma((2, nj)),
                dma((nc,)),
                dma((2,)),
                dma((2, 2, nc)),
                dma((2, 2, nc)),
                dma((2, n - 1, nc)),
                dma((2, n - 1, nc)),
                pltpu.SemaphoreType.REGULAR,
            ],
            compiler_params=pltpu.CompilerParams(
                collective_id=0, has_side_effects=True, vmem_limit_bytes=46 * 2**20
            ),
        )(x, w_gate, w_up, w_down)
        return pl.pallas_call(
            functools.partial(place_kernel, n),
            name="place",
            out_shape=jax.ShapeDtypeStruct((rows, cols), bf16),
            in_specs=[pl.BlockSpec(memory_space=pltpu.VMEM)],
            out_specs=pl.BlockSpec(memory_space=pl.ANY),
            scratch_shapes=[dma((2 * n * cols // FB,))],
            compiler_params=pltpu.CompilerParams(vmem_limit_bytes=2**20),
        )(held)

    return jax.shard_map(
        step,
        mesh=mesh,
        in_specs=(P("dp", None), P(None, "tp"), P(None, "tp"), P("tp", None)),
        out_specs=P("dp", None),
        check_vma=False,
    )
```

```python
import functools

import jax
import jax.numpy as jnp
from jax import lax
from jax.experimental import pallas as pl
from jax.experimental.pallas import tpu as pltpu
from jax.sharding import PartitionSpec as P

MESH = pl.DeviceIdType.MESH
FB = 256
DB = 1024


def ring_kernel(
    n, x, wg, wu, wd, y, right, left, wgv, wuv, wdv, xv, hv, tv, land, out,
    w_sem, d_sem, x_sem, send_rs, recv_rs, send_ag, recv_ag, y_sem,
):
    me = lax.axis_index("tp")
    rows, cols = x.shape
    hidden = wg.shape[1]
    half = rows // 2
    rb = half // n
    nj, nc = hidden // FB, cols // DB
    peers = (lax.rem(me + 1, n), lax.rem(me + n - 1, n))

    def block_rows(d, s):
        b = lax.rem(me + 2 * n - s, n) if d == 0 else lax.rem(me + s, n)
        return pl.ds(pl.multiple_of(d * half + b * rb, rb), rb)

    def columns(i, size):
        return pl.ds(pl.multiple_of(i * size, size), size)

    def load_w(j):
        c = columns(j, FB)
        return (
            pltpu.make_async_copy(wg.at[:, c], wgv.at[:, c], w_sem.at[0, j]),
            pltpu.make_async_copy(wu.at[:, c], wuv.at[:, c], w_sem.at[1, j]),
        )

    def load_d(c):
        k = columns(c, DB)
        return pltpu.make_async_copy(wd.at[:, k], wdv.at[:, k], d_sem.at[c])

    def load_x(d, s):
        return pltpu.make_async_copy(
            x.at[block_rows(d, s), :], xv.at[pl.ds(d * rb, rb), :], x_sem.at[d]
        )

    def remote(src, dst, ssem, rsem, d):
        return pltpu.make_async_remote_copy(
            src_ref=src, dst_ref=dst, send_sem=ssem, recv_sem=rsem,
            device_id={"tp": peers[d]}, device_id_type=MESH,
        )

    def hop(d, s, c):
        now, later = lax.rem(s, 2), lax.rem(s + 1, 2)
        return remote(
            out.at[d, now, c], land.at[d, later, c],
            send_rs.at[d, now, c], recv_rs.at[d, later, c], d,
        )

    def gather_hop(d, t, c):
        there = y.at[block_rows(d, n - 1 + t), columns(c, DB)]
        return remote(there, there, send_ag.at[d, t, c], recv_ag.at[d, t, c], d)

    def first_gather_hop(d, c):
        there = y.at[block_rows(d, n - 1), columns(c, DB)]
        return remote(
            out.at[d, (n - 1) % 2, c], there, send_ag.at[d, 0, c], recv_ag.at[d, 0, c], d
        )

    def side_hop(d, c):
        t = n - 3
        here = y.at[block_rows(d, n - 1 + t), columns(c, DB)]
        there = (right, left)[d].at[:, columns(c, DB)]
        return remote(here, there, send_ag.at[d, t, c], recv_ag.at[d, t, c], d)

    def keep(d, c):
        return pltpu.make_async_copy(
            out.at[d, (n - 1) % 2, c],
            y.at[block_rows(d, n - 1), columns(c, DB)],
            y_sem.at[d, c],
        )

    for d in range(2):
        load_x(d, 0).start()
    for j in range(2):
        for copy in load_w(j):
            copy.start()

    barrier = pltpu.get_barrier_semaphore()
    for peer in peers:
        pl.semaphore_signal(barrier, inc=1, device_id={"tp": peer}, device_id_type=MESH)
    pl.semaphore_wait(barrier, 2)

    def ring_step(s, _):
        for d in range(2):
            load_x(d, s).wait()

        def gate_up(j, _):
            @pl.when(s == 0)
            def _():
                for copy in load_w(j):
                    copy.wait()

                @pl.when(j + 2 < nj)
                def _():
                    for copy in load_w(j + 2):
                        copy.start()

                @pl.when(j + 2 >= nj)
                def _():
                    for i in range(nc // 2):
                        load_d((j + 2 - nj) * (nc // 2) + i).start()

            k = columns(j, FB)
            gate = jnp.dot(xv[...], wgv[:, k], preferred_element_type=jnp.float32)
            up = jnp.dot(xv[...], wuv[:, k], preferred_element_type=jnp.float32)
            hv[:, k] = (jax.nn.silu(gate) * up).astype(jnp.bfloat16)
            return 0

        lax.fori_loop(0, nj, gate_up, 0)

        @pl.when(s < n - 1)
        def _():
            for d in range(2):
                load_x(d, s + 1).start()

        now = lax.rem(s, 2)

        def down(c, _):
            @pl.when(s == 0)
            def _():
                load_d(c).wait()

            tv[...] = jnp.dot(hv[...], wdv[:, columns(c, DB)], preferred_element_type=jnp.float32)

            @pl.when(s >= 2)
            def _():
                for d in range(2):
                    hop(d, s - 2, c).wait_send()

            @pl.when(s == 0)
            def _():
                for d in range(2):
                    out[d, now, c] = tv[d * rb:(d + 1) * rb, :].astype(jnp.bfloat16)

            @pl.when(s > 0)
            def _():
                for d in range(2):
                    hop(d, s - 1, c).wait_recv()
                for d in range(2):
                    total = land[d, now, c].astype(jnp.float32) + tv[d * rb:(d + 1) * rb, :]
                    out[d, now, c] = total.astype(jnp.bfloat16)

            @pl.when(s < n - 1)
            def _():
                for d in range(2):
                    hop(d, s, c).start()

            @pl.when(s == n - 1)
            def _():
                for d in range(2):
                    first_gather_hop(d, c).start()
                for d in range(2):
                    keep(d, c).start()

            return 0

        lax.fori_loop(0, nc, down, 0)
        return 0

    lax.fori_loop(0, n, ring_step, 0)

    def gather_step(t, _):
        def piece(c, _):
            for d in range(2):
                gather_hop(d, t, c).wait_recv()
                gather_hop(d, t + 1, c).start()
            return 0

        return lax.fori_loop(0, nc, piece, 0)

    lax.fori_loop(0, n - 4, gather_step, 0)

    def aside(c, _):
        for d in range(2):
            gather_hop(d, n - 4, c).wait_recv()
            side_hop(d, c).start()
        return 0

    lax.fori_loop(0, nc, aside, 0)

    def finish(c, _):
        for d in range(2):
            hop(d, n - 2, c).wait_send()
            first_gather_hop(d, c).wait_send()
            keep(d, c).wait()

            def sent(t, _):
                gather_hop(d, t, c).wait_send()
                return 0

            lax.fori_loop(1, n - 3, sent, 0)
        return 0

    lax.fori_loop(0, nc, finish, 0)

    def arrive(c, _):
        for d in range(2):
            side_hop(d, c).wait()
        return 0

    lax.fori_loop(0, nc, arrive, 0)


def place_kernel(n, ring, right, left, y, buf, in_sem, out_sem):
    me = lax.axis_index("tp")
    half = y.shape[0] // 2
    rb = half // n

    def at(d, s):
        b = lax.rem(me + 3 * n - s, n) if d == 0 else lax.rem(me + s, n)
        return pl.ds(pl.multiple_of(d * half + b * rb, rb), rb)

    def copy_in(d, i):
        return pltpu.make_async_copy(ring.at[at(d, n - 1 + i), :], buf.at[d, i], in_sem.at[d, i])

    def copy_out(d, i):
        return pltpu.make_async_copy(buf.at[d, i], y.at[at(d, n - 1 + i), :], out_sem.at[d, i])

    def copy_side(d):
        return pltpu.make_async_copy(
            (right, left)[d], y.at[at(d, 2 * n - 3), :], out_sem.at[d, n - 2]
        )

    for i in range(n - 2):
        for d in range(2):
            copy_in(d, i).start()
    for d in range(2):
        copy_side(d).start()
    for i in range(n - 2):
        for d in range(2):
            copy_in(d, i).wait()
            copy_out(d, i).start()
    for d in range(2):
        for i in range(n - 2):
            copy_out(d, i).wait()
        copy_side(d).wait()


def place_last_kernel(n, _, right, left, y, sem):
    me = lax.axis_index("tp")
    half = y.shape[0] // 2
    rb = half // n
    copies = []
    for d in range(2):
        b = lax.rem(me + n + 2, n) if d == 0 else lax.rem(me + n - 2, n)
        copies.append(
            pltpu.make_async_copy(
                (right, left)[d],
                y.at[pl.ds(pl.multiple_of(d * half + b * rb, rb), rb), :],
                sem.at[d],
            )
        )
    for copy in copies:
        copy.start()
    for copy in copies:
        copy.wait()


def solution(mesh):
    n = mesh.shape["tp"]

    def step(x, w_gate, w_up, w_down):
        rows, cols = x.shape
        hidden = w_gate.shape[1]
        rb = rows // 2 // n
        nj, nc = hidden // FB, cols // DB
        dma = pltpu.SemaphoreType.DMA
        bf16 = jnp.bfloat16
        vmem, anywhere = pl.BlockSpec(memory_space=pltpu.VMEM), pl.BlockSpec(memory_space=pl.ANY)
        whole = jax.ShapeDtypeStruct((rows, cols), bf16)
        ring, right, left = pl.pallas_call(
            functools.partial(ring_kernel, n),
            name="mlp_ring",
            out_shape=(whole, pltpu.VMEM((rb, cols), bf16), pltpu.VMEM((rb, cols), bf16)),
            in_specs=[anywhere] * 4,
            out_specs=(anywhere, vmem, vmem),
            scratch_shapes=[
                pltpu.VMEM(w_gate.shape, jnp.bfloat16),
                pltpu.VMEM(w_up.shape, jnp.bfloat16),
                pltpu.VMEM(w_down.shape, jnp.bfloat16),
                pltpu.VMEM((2 * rb, cols), jnp.bfloat16),
                pltpu.VMEM((2 * rb, hidden), jnp.bfloat16),
                pltpu.VMEM((2 * rb, DB), jnp.float32),
                pltpu.VMEM((2, 2, nc, rb, DB), jnp.bfloat16),
                pltpu.VMEM((2, 2, nc, rb, DB), jnp.bfloat16),
                dma((2, nj)),
                dma((nc,)),
                dma((2,)),
                dma((2, 2, nc)),
                dma((2, 2, nc)),
                dma((2, n - 1, nc)),
                dma((2, n - 1, nc)),
                dma((2, nc)),
            ],
            compiler_params=pltpu.CompilerParams(
                collective_id=0, has_side_effects=True, vmem_limit_bytes=61 * 2**20 + 2**19
            ),
        )(x, w_gate, w_up, w_down)
        on_right = lax.ppermute(right, "tp", [(i, (i + 1) % n) for i in range(n)])
        on_left = lax.ppermute(left, "tp", [(i, (i + n - 1) % n) for i in range(n)])
        y = pl.pallas_call(
            functools.partial(place_kernel, n),
            name="place",
            out_shape=whole,
            in_specs=[anywhere, vmem, vmem],
            out_specs=anywhere,
            scratch_shapes=[pltpu.VMEM((2, n - 2, rb, cols), bf16), dma((2, n - 2)), dma((2, n - 1))],
            compiler_params=pltpu.CompilerParams(vmem_limit_bytes=50 * 2**20),
            cost_estimate=pl.CostEstimate(
                flops=0, bytes_accessed=4 * rows * cols, transcendentals=0
            ),
        )(ring, right, left)
        return pl.pallas_call(
            functools.partial(place_last_kernel, n),
            name="place_last",
            out_shape=whole,
            in_specs=[anywhere, vmem, vmem],
            out_specs=anywhere,
            input_output_aliases={0: 0},
            scratch_shapes=[dma((2,))],
            compiler_params=pltpu.CompilerParams(vmem_limit_bytes=50 * 2**20),
        )(y, on_right, on_left)

    return jax.shard_map(
        step,
        mesh=mesh,
        in_specs=(P("dp", None), P(None, "tp"), P(None, "tp"), P("tp", None)),
        out_specs=P("dp", None),
        check_vma=False,
    )
```

```python
import functools

import jax
import jax.numpy as jnp
from jax import lax
from jax.experimental import pallas as pl
from jax.experimental.pallas import tpu as pltpu
from jax.sharding import PartitionSpec as P

MESH = pl.DeviceIdType.MESH
FB = 256
DB = 1024


def ring_kernel(
    n, x, wg, wu, wd, y, right, left, wgv, wuv, wdv, xv, hv, tv, land, out,
    w_sem, d_sem, x_sem, send_rs, recv_rs, send_ag, recv_ag, y_sem,
):
    me = lax.axis_index("tp")
    rows, cols = x.shape
    hidden = wg.shape[1]
    half = rows // 2
    rb = half // n
    nj, nc = hidden // FB, cols // DB
    peers = (lax.rem(me + 1, n), lax.rem(me + n - 1, n))

    def block_rows(d, s):
        b = lax.rem(me + 2 * n - s, n) if d == 0 else lax.rem(me + s, n)
        return pl.ds(pl.multiple_of(d * half + b * rb, rb), rb)

    def columns(i, size):
        return pl.ds(pl.multiple_of(i * size, size), size)

    def load_w(j):
        c = columns(j, FB)
        return (
            pltpu.make_async_copy(wg.at[:, c], wgv.at[:, c], w_sem.at[0, j]),
            pltpu.make_async_copy(wu.at[:, c], wuv.at[:, c], w_sem.at[1, j]),
        )

    def load_d(c):
        k = columns(c, DB)
        return pltpu.make_async_copy(wd.at[:, k], wdv.at[:, k], d_sem.at[c])

    def load_x(d, s):
        return pltpu.make_async_copy(
            x.at[block_rows(d, s), :], xv.at[pl.ds(d * rb, rb), :], x_sem.at[d]
        )

    def remote(src, dst, ssem, rsem, d):
        return pltpu.make_async_remote_copy(
            src_ref=src, dst_ref=dst, send_sem=ssem, recv_sem=rsem,
            device_id={"tp": peers[d]}, device_id_type=MESH,
        )

    def hop(d, s, c):
        now, later = lax.rem(s, 2), lax.rem(s + 1, 2)
        return remote(
            out.at[d, now, c], land.at[d, later, c],
            send_rs.at[d, now, c], recv_rs.at[d, later, c], d,
        )

    def gather_hop(d, t, c):
        there = y.at[block_rows(d, n - 1 + t), columns(c, DB)]
        return remote(there, there, send_ag.at[d, t, c], recv_ag.at[d, t, c], d)

    def first_gather_hop(d, c):
        there = y.at[block_rows(d, n - 1), columns(c, DB)]
        return remote(
            out.at[d, (n - 1) % 2, c], there, send_ag.at[d, 0, c], recv_ag.at[d, 0, c], d
        )

    def side_hop(d, c):
        t = n - 3
        here = y.at[block_rows(d, n - 1 + t), columns(c, DB)]
        there = (right, left)[d].at[:, columns(c, DB)]
        return remote(here, there, send_ag.at[d, t, c], recv_ag.at[d, t, c], d)

    def keep(d, c):
        return pltpu.make_async_copy(
            out.at[d, (n - 1) % 2, c],
            y.at[block_rows(d, n - 1), columns(c, DB)],
            y_sem.at[d, c],
        )

    for d in range(2):
        load_x(d, 0).start()
    for copy in load_w(0):
        copy.start()

    barrier = pltpu.get_barrier_semaphore()
    for peer in peers:
        pl.semaphore_signal(barrier, inc=1, device_id={"tp": peer}, device_id_type=MESH)
    pl.semaphore_wait(barrier, 2)

    def ring_step(s, _):
        for d in range(2):
            load_x(d, s).wait()

        @pl.when(s == 0)
        def _():
            for copy in load_w(1):
                copy.start()

        def gate_up(j, _):
            @pl.when(s == 0)
            def _():
                for copy in load_w(j):
                    copy.wait()

                @pl.when(j + 2 < nj)
                def _():
                    for copy in load_w(j + 2):
                        copy.start()

                @pl.when(j + 2 >= nj)
                def _():
                    for i in range(nc // 2):
                        load_d((j + 2 - nj) * (nc // 2) + i).start()

            k = columns(j, FB)
            gate = jnp.dot(xv[...], wgv[:, k], preferred_element_type=jnp.float32)
            up = jnp.dot(xv[...], wuv[:, k], preferred_element_type=jnp.float32)
            hv[:, k] = (jax.nn.silu(gate) * up).astype(jnp.bfloat16)
            return 0

        lax.fori_loop(0, nj, gate_up, 0)

        @pl.when(s < n - 1)
        def _():
            for d in range(2):
                load_x(d, s + 1).start()

        now = lax.rem(s, 2)

        def down(c, _):
            @pl.when(s == 0)
            def _():
                load_d(c).wait()

            tv[...] = jnp.dot(hv[...], wdv[:, columns(c, DB)], preferred_element_type=jnp.float32)

            @pl.when(s >= 2)
            def _():
                for d in range(2):
                    hop(d, s - 2, c).wait_send()

            @pl.when(s == 0)
            def _():
                for d in range(2):
                    out[d, now, c] = tv[d * rb:(d + 1) * rb, :].astype(jnp.bfloat16)

            @pl.when(s > 0)
            def _():
                for d in range(2):
                    hop(d, s - 1, c).wait_recv()
                for d in range(2):
                    total = land[d, now, c].astype(jnp.float32) + tv[d * rb:(d + 1) * rb, :]
                    out[d, now, c] = total.astype(jnp.bfloat16)

            @pl.when(s < n - 1)
            def _():
                for d in range(2):
                    hop(d, s, c).start()

            @pl.when(s == n - 1)
            def _():
                for d in range(2):
                    first_gather_hop(d, c).start()
                for d in range(2):
                    keep(d, c).start()

            return 0

        lax.fori_loop(0, nc, down, 0)
        return 0

    lax.fori_loop(0, n, ring_step, 0)

    def gather_step(t, _):
        def piece(c, _):
            for d in range(2):
                gather_hop(d, t, c).wait_recv()
                gather_hop(d, t + 1, c).start()
            return 0

        return lax.fori_loop(0, nc, piece, 0)

    lax.fori_loop(0, n - 4, gather_step, 0)

    def aside(c, _):
        for d in range(2):
            gather_hop(d, n - 4, c).wait_recv()
            side_hop(d, c).start()
        return 0

    lax.fori_loop(0, nc, aside, 0)

    def finish(c, _):
        for d in range(2):
            hop(d, n - 2, c).wait_send()
            first_gather_hop(d, c).wait_send()
            keep(d, c).wait()

            def sent(t, _):
                gather_hop(d, t, c).wait_send()
                return 0

            lax.fori_loop(1, n - 3, sent, 0)
        return 0

    lax.fori_loop(0, nc, finish, 0)

    def arrive(c, _):
        for d in range(2):
            side_hop(d, c).wait()
        return 0

    lax.fori_loop(0, nc, arrive, 0)


def place_kernel(n, ring, right, left, y, buf, in_sem, out_sem):
    me = lax.axis_index("tp")
    half = y.shape[0] // 2
    rb = half // n

    def at(d, s):
        b = lax.rem(me + 3 * n - s, n) if d == 0 else lax.rem(me + s, n)
        return pl.ds(pl.multiple_of(d * half + b * rb, rb), rb)

    def copy_in(d, i):
        return pltpu.make_async_copy(ring.at[at(d, n - 1 + i), :], buf.at[d, i], in_sem.at[d, i])

    def copy_out(d, i):
        return pltpu.make_async_copy(buf.at[d, i], y.at[at(d, n - 1 + i), :], out_sem.at[d, i])

    def copy_side(d):
        return pltpu.make_async_copy(
            (right, left)[d], y.at[at(d, 2 * n - 3), :], out_sem.at[d, n - 2]
        )

    for i in range(n - 2):
        for d in range(2):
            copy_in(d, i).start()
    for d in range(2):
        copy_side(d).start()
    for i in range(n - 2):
        for d in range(2):
            copy_in(d, i).wait()
            copy_out(d, i).start()
    for d in range(2):
        for i in range(n - 2):
            copy_out(d, i).wait()
        copy_side(d).wait()


def place_last_kernel(n, _, right, left, y, sem):
    me = lax.axis_index("tp")
    half = y.shape[0] // 2
    rb = half // n
    copies = []
    for d in range(2):
        b = lax.rem(me + n + 2, n) if d == 0 else lax.rem(me + n - 2, n)
        copies.append(
            pltpu.make_async_copy(
                (right, left)[d],
                y.at[pl.ds(pl.multiple_of(d * half + b * rb, rb), rb), :],
                sem.at[d],
            )
        )
    for copy in copies:
        copy.start()
    for copy in copies:
        copy.wait()


def solution(mesh):
    n = mesh.shape["tp"]

    def step(x, w_gate, w_up, w_down):
        rows, cols = x.shape
        hidden = w_gate.shape[1]
        rb = rows // 2 // n
        nj, nc = hidden // FB, cols // DB
        dma = pltpu.SemaphoreType.DMA
        bf16 = jnp.bfloat16
        vmem, anywhere = pl.BlockSpec(memory_space=pltpu.VMEM), pl.BlockSpec(memory_space=pl.ANY)
        whole = jax.ShapeDtypeStruct((rows, cols), bf16)
        ring, right, left = pl.pallas_call(
            functools.partial(ring_kernel, n),
            name="mlp_ring",
            out_shape=(whole, pltpu.VMEM((rb, cols), bf16), pltpu.VMEM((rb, cols), bf16)),
            in_specs=[anywhere] * 4,
            out_specs=(anywhere, vmem, vmem),
            scratch_shapes=[
                pltpu.VMEM(w_gate.shape, jnp.bfloat16),
                pltpu.VMEM(w_up.shape, jnp.bfloat16),
                pltpu.VMEM(w_down.shape, jnp.bfloat16),
                pltpu.VMEM((2 * rb, cols), jnp.bfloat16),
                pltpu.VMEM((2 * rb, hidden), jnp.bfloat16),
                pltpu.VMEM((2 * rb, DB), jnp.float32),
                pltpu.VMEM((2, 2, nc, rb, DB), jnp.bfloat16),
                pltpu.VMEM((2, 2, nc, rb, DB), jnp.bfloat16),
                dma((2, nj)),
                dma((nc,)),
                dma((2,)),
                dma((2, 2, nc)),
                dma((2, 2, nc)),
                dma((2, n - 1, nc)),
                dma((2, n - 1, nc)),
                dma((2, nc)),
            ],
            compiler_params=pltpu.CompilerParams(
                collective_id=0, has_side_effects=True, vmem_limit_bytes=61 * 2**20 + 2**19
            ),
        )(x, w_gate, w_up, w_down)
        on_right = lax.ppermute(right, "tp", [(i, (i + 1) % n) for i in range(n)])
        on_left = lax.ppermute(left, "tp", [(i, (i + n - 1) % n) for i in range(n)])
        y = pl.pallas_call(
            functools.partial(place_kernel, n),
            name="place",
            out_shape=whole,
            in_specs=[anywhere, vmem, vmem],
            out_specs=anywhere,
            scratch_shapes=[pltpu.VMEM((2, n - 2, rb, cols), bf16), dma((2, n - 2)), dma((2, n - 1))],
            compiler_params=pltpu.CompilerParams(vmem_limit_bytes=50 * 2**20),
            cost_estimate=pl.CostEstimate(
                flops=0, bytes_accessed=4 * rows * cols, transcendentals=0
            ),
        )(ring, right, left)
        return pl.pallas_call(
            functools.partial(place_last_kernel, n),
            name="place_last",
            out_shape=whole,
            in_specs=[anywhere, vmem, vmem],
            out_specs=anywhere,
            input_output_aliases={0: 0},
            scratch_shapes=[dma((2,))],
            compiler_params=pltpu.CompilerParams(vmem_limit_bytes=50 * 2**20),
        )(y, on_right, on_left)

    return jax.shard_map(
        step,
        mesh=mesh,
        in_specs=(P("dp", None), P(None, "tp"), P(None, "tp"), P("tp", None)),
        out_specs=P("dp", None),
        check_vma=False,
    )
```
